16 devices in a mesh: dp: 4 (over y, z, core), sp: 4 (over x).
Axes of the slice: x: 4, y: 2, z: 1, core: 2. Of those that a mesh axis runs over, the one named last changes fastest.
The devices are a block of a 4x4x8 slice.
Arguments:
- x: bfloat16 [2048, 4096], P(('dp', 'sp')), parts along dimension 0
- gain: bfloat16 [4096], replicated
- wq: bfloat16 [4096, 4096], replicated
- wk: bfloat16 [4096, 512], replicated
- wv: bfloat16 [4096, 512], replicated
- wo: bfloat16 [4096, 4096], replicated
Outputs:
- output: bfloat16 [2048, 4096], P(('dp', 'sp')), parts along dimension 0
There are 4 independent parts. The reference program is written for one: setup_inputs(seed, part) draws one part's arguments, and reference() takes and returns one part's arrays. A program takes and returns all parts, laid end to end along the dimension named above; an argument that names none is the same for every part.
All inputs are finite; a program needn't handle non-finite values.
Results may differ from the reference program's by a relative error of at most 0.012.
Values are sent between devices in bfloat16 or wider.
A program may use at most 768 MiB of HBM per device.

```python
import jax
import jax.numpy as jnp
from jax import lax

ROWS = 512
D = 4096
HEADS = 32
KV_HEADS = 4
HEAD = 128
THETA = 10000


def setup_inputs(seed: int = 0, part: int = 0) -> dict:
    kx, kn, kq, kk, kv, ko = jax.random.split(jax.random.key(seed), 6)

    def weights(key, rows, columns):
        return jax.random.normal(key, (rows, columns), jnp.float32) * rows**-0.5

    drawn = {
        "x": jax.random.normal(jax.random.fold_in(kx, part), (ROWS, D), jnp.float32),
        "gain": 1 + 0.1 * jax.random.normal(kn, (D,), jnp.float32),
        "wq": 2 * weights(kq, D, HEADS * HEAD),
        "wk": 2 * weights(kk, D, KV_HEADS * HEAD),
        "wv": 4 * weights(kv, D, KV_HEADS * HEAD),
        "wo": weights(ko, HEADS * HEAD, D),
    }
    return {k: v.astype(jnp.bfloat16) for k, v in drawn.items()}


def normed(x, gain):
    wide = x.astype(jnp.float32)
    scale = lax.rsqrt(jnp.mean(wide * wide, -1, keepdims=True) + 1e-6)
    return (wide * scale * gain.astype(jnp.float32)).astype(jnp.bfloat16)


def turned(t, place, theta):
    half = t.shape[-1] // 2
    angle = place.astype(jnp.float32)[:, None] * theta ** (-jnp.arange(half, dtype=jnp.float32) / half)
    cos, sin = jnp.cos(angle)[:, None], jnp.sin(angle)[:, None]
    a, b = t[..., :half].astype(jnp.float32), t[..., half:].astype(jnp.float32)
    return jnp.concatenate([a * cos - b * sin, b * cos + a * sin], -1).astype(jnp.bfloat16)


def matmul(a, w):
    return jnp.dot(a, w, preferred_element_type=jnp.float32).astype(jnp.bfloat16)


def einsum(form, a, b):
    return jnp.einsum(form, a.astype(jnp.float32), b.astype(jnp.float32))


def attention(q, k, v):
    scores = einsum("tgsd,ugd->gstu", q, k) * q.shape[-1] ** -0.5
    token = jnp.arange(q.shape[0])
    scores = jnp.where(token[:, None] >= token, scores, -jnp.inf)
    weights = jax.nn.softmax(scores, -1).astype(jnp.bfloat16)
    return einsum("gstu,ugd->tgsd", weights, v).astype(jnp.bfloat16)


def reference(x, gain, wq, wk, wv, wo):
    a, place = normed(x, gain), jnp.arange(ROWS)
    q = turned(matmul(a, wq).reshape(ROWS, HEADS, HEAD), place, THETA).reshape(ROWS, KV_HEADS, -1, HEAD)
    k = turned(matmul(a, wk).reshape(ROWS, KV_HEADS, HEAD), place, THETA)
    v = matmul(a, wv).reshape(ROWS, KV_HEADS, HEAD)
    seen = attention(q, k, v).reshape(ROWS, HEADS * HEAD)
    return (x.astype(jnp.float32) + jnp.dot(seen, wo, preferred_element_type=jnp.float32)).astype(jnp.bfloat16)
```

```python
import functools

import jax
import jax.numpy as jnp
import numpy as np
from jax import lax
from jax.experimental import pallas as pl
from jax.experimental.pallas import tpu as pltpu
from jax.sharding import PartitionSpec as P

HEAD = 128
THETA = 10000
LOG2E = 1.4426950408889634
MESH = pl.DeviceIdType.MESH
LANES = 128
SLOTS = 4


def tables(tokens):
    half = HEAD // 2
    rate = np.float32(THETA) ** (-np.arange(half, dtype=np.float32) / np.float32(half))
    angle = (np.arange(tokens, dtype=np.float32)[:, None] * rate.astype(np.float32)).astype(np.float64)
    cos, sin = np.cos(angle).astype(np.float32), np.sin(angle).astype(np.float32)
    return np.concatenate([cos, cos, -sin, sin], -1)


def dot(a, b, ca=1, cb=0):
    return lax.dot_general(a, b, (((ca,), (cb,)), ((), ())), preferred_element_type=jnp.float32)


def kernel(n, x_hbm, gain_hbm, turn_hbm, wq_hbm, wk_hbm, wv_hbm, wo_hbm, y_hbm,
           x, gain, turn, a, w, wo, q, kv, cap, seen, total, out,
           in_sem, w_sem, wo_sem, out_sem, send_sem, relay_sem, recv_sem):
    me = lax.axis_index("sp")
    own, width = x.shape
    kv_heads = kv.shape[0]
    per = q.shape[0] // (kv_heads * own)
    chunk = w.shape[2]
    q_chunks = wq_hbm.shape[1] // chunk
    part = chunk // 2
    wo_rows = wo.shape[0] // (2 * kv_heads)

    def place(*refs):
        return pltpu.make_async_copy(*refs)

    inputs = [
        place(x_hbm, x, in_sem.at[0]),
        place(gain_hbm, gain, in_sem.at[1]),
        place(turn_hbm.at[pl.ds(pl.multiple_of(me * own, own), own)], turn, in_sem.at[2]),
    ]
    for c in inputs:
        c.start()

    def w_copy(i, half):
        src = (wk_hbm, wv_hbm)[i] if i < 2 else wq_hbm
        at = half * part + (0 if i < 2 else (i - 2) * chunk)
        return place(src.at[:, pl.ds(at, part)], w.at[i % SLOTS, :, pl.ds(half * part, part)], w_sem.at[i, half])

    for half in range(2):
        for i in range(2):
            w_copy(i, half).start()
    for i in range(2, SLOTS):
        for half in range(2):
            w_copy(i, half).start()

    def wo_copy(i):
        rows = pl.ds(i * wo_rows, wo_rows)
        return place(wo_hbm.at[rows, :], wo.at[rows, :], wo_sem.at[i])

    barrier = pltpu.get_barrier_semaphore()
    for step in range(1, n):
        pl.semaphore_signal(barrier, inc=1, device_id={"sp": lax.rem(me + step, n)}, device_id_type=MESH)

    tokens = n * own
    for j in range(1, n):
        for h in range(kv_heads):
            relayed = j == 1 and h % 2 == 1 and n > 3
            @pl.when(me < j if not relayed else (me < j) & (me != 0))
            def _():
                kv[h, pl.ds(j * own, own), :] = jnp.zeros((own, 2 * HEAD), kv.dtype)
    place_q = me * own + lax.broadcasted_iota(jnp.int32, (own, tokens), 0)
    place_k = lax.broadcasted_iota(jnp.int32, (own, tokens), 1)
    cap[...] = jnp.where(place_q >= place_k, jnp.inf, -jnp.inf)

    for c in inputs:
        c.wait()
    cols = [slice(i * LANES, (i + 1) * LANES) for i in range(width // LANES)]
    square = jnp.zeros((own, LANES), jnp.float32)
    for s in cols:
        wide = x[:, s].astype(jnp.float32)
        square += wide * wide
    scale = lax.rsqrt(jnp.sum(square, -1, keepdims=True) * (1 / width) + 1e-6)
    for i, s in enumerate(cols):
        a[:, s] = (x[:, s].astype(jnp.float32) * scale * gain[i : i + 1, :].astype(jnp.float32)).astype(a.dtype)

    def turned(t):
        t = t.astype(jnp.bfloat16).astype(jnp.float32)
        return (t * turn[:, :HEAD] + pltpu.roll(t, HEAD // 2, 1) * turn[:, HEAD:]).astype(jnp.bfloat16)

    def block(h, j):
        return kv.at[h, pl.ds(j * own if isinstance(j, int) else pl.multiple_of(j * own, own), own), :]

    def send(h, j, to, sem):
        return pltpu.make_async_remote_copy(src_ref=block(h, j), dst_ref=block(h, j), send_sem=sem, recv_sem=recv_sem.at[h, j],
                                            device_id={"sp": to}, device_id_type=MESH)

    hops = [(j, j + 1) for j in range(n - 1)] + [(0, n - 1)]
    per_round = part // HEAD

    for half in range(2):
        for i in range(2):
            w_copy(i, half).wait()
        at = pl.ds(half * part, part)
        k2 = dot(a[...], w[0, :, at])
        v2 = dot(a[...], w[1, :, at])
        for u in range(per_round):
            h, s = half * per_round + u, slice(u * HEAD, (u + 1) * HEAD)
            rows = pl.ds(pl.multiple_of(me * own, own), own)
            kv[h, rows, :HEAD] = turned(k2[:, s])
            kv[h, rows, HEAD:] = v2[:, s].astype(jnp.bfloat16)
        if half == 0:
            pl.semaphore_wait(barrier, n - 1)
        for j, to in hops:
            @pl.when(me == j)
            def _():
                for u in range(per_round):
                    h = half * per_round + u
                    send(h, j, to, send_sem.at[h, to]).start()
        @pl.when(me == 1)
        def _():
            for u in range(per_round):
                h = half * per_round + u
                if h % 2 == 1:
                    send(h, 1, 0, send_sem.at[h, 0]).start()

    relays = [(n - 1, 0, 2, range(kv_heads)), (2, 1, n - 1, range(0, kv_heads, 2)), (0, 1, n - 1, range(1, kv_heads, 2))]

    def relay(h):
        for via, j, to, heads in relays:
            if h in heads:
                @pl.when(me == via)
                def _():
                    send(h, j, to, relay_sem.at[h]).wait_recv()
                    send(h, j, to, relay_sem.at[h]).start()

    chunks = 2 + q_chunks

    def fetch(i):
        if i < chunks:
            for half in range(2):
                w_copy(i, half).start()
        if i == chunks:
            for c in range(2 * kv_heads):
                wo_copy(c).start()

    fetch(SLOTS)
    fetch(SLOTS + 1)
    relay_after = {3: [0], 4: [1], 5: [2], 7: [3]}
    for i in range(2, chunks):
        for half in range(2):
            w_copy(i, half).wait()
        t = dot(a[...], w[i % SLOTS])
        for u in range(chunk // HEAD):
            h = (i - 2) * (chunk // HEAD) + u
            q[h * own : (h + 1) * own, :] = turned(t[:, u * HEAD : (u + 1) * HEAD])
        fetch(i + SLOTS)
        for h in relay_after.get(i - 2, []):
            relay(h)

    e = HEAD**-0.5 * LOG2E
    heads_at_once = 2
    strip = heads_at_once * own
    n_cols = 512
    for g in range(kv_heads):
        for j in range(n - 1):
            @pl.when(me > j)
            def _():
                done = [via for via, b, _, heads in relays if b == j and g in heads]
                ok = me >= 0
                for via in done:
                    ok = ok & (me != via)
                @pl.when(ok)
                def _():
                    send(g, j, lax.rem(me + 1, n), relay_sem.at[g]).wait_recv()
        keys = kv[g, :, :HEAD]
        values = jnp.concatenate([kv[g, :, HEAD:], jnp.ones((tokens, HEAD), kv.dtype)], axis=1)
        for u in range(per // heads_at_once):
            first = (g * per + u * heads_at_once) * own
            s = dot(q[first : first + strip, :], keys, 1, 1)
            s = jnp.minimum(s, jnp.concatenate([cap[...]] * heads_at_once, axis=0))
            top = jnp.max(s, -1, keepdims=True)
            p = jnp.exp2((s - top) * e).astype(jnp.bfloat16)
            o = dot(p, values)
            o = (o[:, :HEAD] / o[:, HEAD:]).astype(jnp.bfloat16)
            for k in range(heads_at_once):
                h = u * heads_at_once + k
                seen[:, h * HEAD : (h + 1) * HEAD] = o[k * own : (k + 1) * own, :]
        for i in range(2):
            wo_copy(2 * g + i).wait()
        rows = pl.ds(g * 2 * wo_rows, 2 * wo_rows)
        for c in range(width // n_cols):
            s = pl.ds(c * n_cols, n_cols)
            t = dot(seen[...], wo[rows, s])
            if g == 0:
                total[:, s] = t
            elif g < kv_heads - 1:
                total[:, s] += t
            else:
                out[:, s] = (x[:, s].astype(jnp.float32) + (total[:, s] + t)).astype(out.dtype)
                place(out.at[:, s], y_hbm.at[:, s], out_sem.at[c]).start()

    for c in range(width // n_cols):
        s = pl.ds(c * n_cols, n_cols)
        place(out.at[:, s], y_hbm.at[:, s], out_sem.at[c]).wait()
    for h in range(kv_heads):
        for j, to in hops + ([(1, 0)] if h % 2 == 1 else []):
            @pl.when(me == j)
            def _():
                send(h, j, to, send_sem.at[h, to]).wait_send()
        for via, j, to, heads in relays:
            if h in heads:
                @pl.when(me == via)
                def _():
                    send(h, j, to, relay_sem.at[h]).wait_send()


def solution(mesh):
    n = mesh.shape["sp"]

    def step(x, gain, wq, wk, wv, wo):
        own, width = x.shape
        kv_heads, heads = wk.shape[1] // HEAD, wq.shape[1] // HEAD
        chunk = wk.shape[1]
        q_chunks = wq.shape[1] // chunk
        tokens = n * own
        anywhere = pl.BlockSpec(memory_space=pltpu.HBM)
        weights = sum(t.size for t in (wq, wk, wv, wo))
        vmem, f32, bf16, dma = pltpu.VMEM, jnp.float32, jnp.bfloat16, pltpu.SemaphoreType.DMA
        return pl.pallas_call(
            functools.partial(kernel, n),
            out_shape=jax.ShapeDtypeStruct(x.shape, x.dtype),
            in_specs=[anywhere] * 7,
            out_specs=anywhere,
            scratch_shapes=[
                vmem((own, width), bf16), vmem((width // LANES, LANES), bf16), vmem((own, 2 * HEAD), f32),
                vmem((own, width), bf16), vmem((SLOTS, width, chunk), bf16), vmem(wo.shape, bf16),
                vmem((heads * own, HEAD), bf16), vmem((kv_heads, tokens, 2 * HEAD), bf16), vmem((own, tokens), f32),
                vmem((own, heads // kv_heads * HEAD), bf16), vmem((own, width), f32), vmem((own, width), bf16),
                dma((3,)), dma((2 + q_chunks, 2)), dma((2 * kv_heads,)), dma((width // 512,)), dma((kv_heads, n)), dma((kv_heads,)),
                dma((kv_heads, n)),
            ],
            compiler_params=pltpu.CompilerParams(collective_id=0, has_side_effects=True, vmem_limit_bytes=63 * 2**20),
            cost_estimate=pl.CostEstimate(flops=2 * own * weights, bytes_accessed=2 * weights, transcendentals=heads * own * tokens),
        )(x, gain.reshape(width // LANES, LANES), jnp.asarray(tables(tokens)), wq, wk, wv, wo)

    rows, whole = P(("dp", "sp"), None), P(None, None)
    return jax.shard_map(
        step,
        mesh=mesh,
        in_specs=(rows, P(None), whole, whole, whole, whole),
        out_specs=rows,
        check_vma=False,
    )
```

```python
import functools

import jax
import jax.numpy as jnp
import numpy as np
from jax import lax
from jax.experimental import pallas as pl
from jax.experimental.pallas import tpu as pltpu
from jax.sharding import PartitionSpec as P

HEAD = 128
THETA = 10000
LOG2E = 1.4426950408889634
MESH = pl.DeviceIdType.MESH
LANES = 128
SLOTS = 5
WO_SLOTS = 5
PIECES = 4
N_COLS = 512


def tables(tokens):
    half = HEAD // 2
    rate = np.float32(THETA) ** (-np.arange(half, dtype=np.float32) / np.float32(half))
    angle = (np.arange(tokens, dtype=np.float32)[:, None] * rate.astype(np.float32)).astype(np.float64)
    cos, sin = np.cos(angle).astype(np.float32), np.sin(angle).astype(np.float32)
    return np.concatenate([cos, cos, -sin, sin], -1)


def dot(a, b, ca=1, cb=0):
    return lax.dot_general(a, b, (((ca,), (cb,)), ((), ())), preferred_element_type=jnp.float32)


def kernel(n, x_hbm, gain_hbm, turn_hbm, wq_hbm, wk_hbm, wv_hbm, wo_hbm, y,
           x, gain, turn, a, w, wo, q, q_out, kv, cap, seen, total,
           in_sem, w_sem, wo_sem, send_sem, relay_sem, recv_sem, a_send, a_recv, q_send, q_recv):
    me, group = lax.axis_index("sp"), lax.axis_index("dp")
    side = lax.rem(group, 2)
    partner = {"dp": group + 1 - 2 * side}
    own, width = x.shape
    kv_heads = kv.shape[0]
    heads = q.shape[0] // own
    per = heads // kv_heads
    chunk = w.shape[2]
    q_chunks = heads * HEAD // (2 * chunk)
    chunk_heads = chunk // HEAD
    chunks = 2 + q_chunks
    part = chunk // 2
    wo_rows = wo.shape[1]
    wo_chunks = heads * HEAD // wo_rows
    wo_per = wo_chunks // kv_heads
    tokens = n * own
    order = [lax.rem(kv_heads // 2 * side + k, kv_heads) for k in range(kv_heads)]

    def ds(at, size):
        return pl.ds(at if isinstance(at, int) else pl.multiple_of(at, size), size)

    mine = ds(me * own, own)

    place = pltpu.make_async_copy
    inputs = [
        place(x_hbm, x, in_sem.at[0]),
        place(gain_hbm, gain, in_sem.at[1]),
        place(turn_hbm.at[mine], turn, in_sem.at[2]),
    ]
    for c in inputs:
        c.start()

    def w_copy(i, half):
        if i < 2:
            src, at = (wk_hbm, wv_hbm)[i], ds(lax.rem(side + half, 2) * part, part)
        else:
            src, at = wq_hbm, ds((side * q_chunks + i - 2) * chunk + half * part, part)
        return place(src.at[:, at], w.at[i % SLOTS, :, pl.ds(half * part, part)], w_sem.at[i, half])

    def wo_copy(i):
        rows = ds(order[i // wo_per] * (wo_per * wo_rows) + i % wo_per * wo_rows, wo_rows)
        return place(wo_hbm.at[rows, :], wo.at[i % WO_SLOTS], wo_sem.at[i])

    def fetch(i):
        if i < chunks:
            for half in range(2):
                w_copy(i, half).start(priority=1)

    for half in range(2):
        for i in range(2):
            w_copy(i, half).start(priority=1)
    for i in range(2, SLOTS - 1):
        fetch(i)

    barrier = pltpu.get_barrier_semaphore()
    for step in range(1, n):
        pl.semaphore_signal(barrier, inc=1, device_id={"sp": lax.rem(me + step, n)}, device_id_type=MESH)
    pl.semaphore_signal(barrier, inc=1, device_id=partner, device_id_type=MESH)

    def block(k, j):
        return kv.at[order[k], ds(j * own, own), :]

    for j in range(1, n):
        for k in range(kv_heads):
            relayed = j == 1 and k % 2 == 1
            @pl.when(me < j if not relayed else (me < j) & (me != 0))
            def _():
                block(k, j)[...] = jnp.zeros((own, 2 * HEAD), kv.dtype)
    place_q = me * own + lax.broadcasted_iota(jnp.int32, (own, tokens), 0)
    place_k = lax.broadcasted_iota(jnp.int32, (own, tokens), 1)
    cap[...] = jnp.where(place_q >= place_k, jnp.inf, -jnp.inf)

    for c in inputs:
        c.wait()
    cols = [slice(i * LANES, (i + 1) * LANES) for i in range(width // LANES)]
    square = jnp.zeros((own, LANES), jnp.float32)
    for s in cols:
        wide = x[:, s].astype(jnp.float32)
        square += wide * wide
    scale = lax.rsqrt(jnp.sum(square, -1, keepdims=True) * (1 / width) + 1e-6)
    pl.semaphore_wait(barrier, n)

    def a_copy(i):
        s = pl.ds(i * (width // PIECES), width // PIECES)
        return pltpu.make_async_remote_copy(src_ref=a.at[:own, s], dst_ref=a.at[own:, s], send_sem=a_send.at[i], recv_sem=a_recv.at[i],
                                            device_id=partner, device_id_type=MESH)

    for i, s in enumerate(cols):
        a[:own, s] = (x[:, s].astype(jnp.float32) * scale * gain[i : i + 1, :].astype(jnp.float32)).astype(a.dtype)
        if (i + 1) % (len(cols) // PIECES) == 0:
            a_copy(i // (len(cols) // PIECES)).start()

    def turned(t):
        t = t.astype(jnp.bfloat16).astype(jnp.float32)
        return (t * turn[:, :HEAD] + pltpu.roll(t, HEAD // 2, 1) * turn[:, HEAD:]).astype(jnp.bfloat16)

    def send(k, j, to, sem):
        return pltpu.make_async_remote_copy(src_ref=block(k, j), dst_ref=block(k, j), send_sem=sem, recv_sem=recv_sem.at[k, j],
                                            device_id={"sp": to}, device_id_type=MESH)

    hops = [(j, j + 1, range(kv_heads)) for j in range(n - 1)] + [(0, n - 1, range(kv_heads)), (1, 0, range(1, kv_heads, 2))]
    relays = [(n - 1, 0, 2, range(kv_heads)), (2, 1, n - 1, range(0, kv_heads, 2)), (0, 1, n - 1, range(1, kv_heads, 2))]

    for half in range(2):
        for i in range(2):
            w_copy(i, half).wait()
        at = pl.ds(half * part, part)
        k2 = dot(a[:own], w[0, :, at])
        v2 = dot(a[:own], w[1, :, at])
        ks = [half * (part // HEAD) + u for u in range(part // HEAD)]
        for u, k in enumerate(ks):
            s = slice(u * HEAD, (u + 1) * HEAD)
            kv[order[k], mine, :HEAD] = turned(k2[:, s])
            kv[order[k], mine, HEAD:] = v2[:, s].astype(jnp.bfloat16)
        for j, to, which in hops:
            @pl.when(me == j)
            def _():
                for k in ks:
                    if k in which:
                        send(k, j, to, send_sem.at[k, to]).start()
        fetch(SLOTS - 1 + half)

    def relay(k):
        for via, j, to, which in relays:
            if k in which:
                @pl.when(me == via)
                def _():
                    send(k, j, to, relay_sem.at[k]).wait_recv()
                    send(k, j, to, relay_sem.at[k]).start()

    for i in range(PIECES):
        a_copy(i).wait_recv()

    def q_copy(i, whose):
        rows = pl.ds(i * chunk_heads * own, chunk_heads * own)
        there = ds((whose * q_chunks + i) * (chunk_heads * own), chunk_heads * own)
        return pltpu.make_async_remote_copy(src_ref=q_out.at[rows], dst_ref=q.at[there], send_sem=q_send.at[i], recv_sem=q_recv.at[i],
                                            device_id=partner, device_id_type=MESH)

    for i in range(q_chunks):
        for half in range(2):
            w_copy(2 + i, half).wait()
        t = dot(a[...], w[(2 + i) % SLOTS])
        for u in range(chunk_heads):
            s = slice(u * HEAD, (u + 1) * HEAD)
            h = i * chunk_heads + u
            q_out[h * own : (h + 1) * own, :] = turned(t[own:, s])
            q[ds((side * (heads // 2) + h) * own, own), :] = turned(t[:own, s])
        q_copy(i, side).start()
        for c in ([0, 1], [2], [3], [4])[i]:
            wo_copy(c).start(priority=1)
        if i > 0:
            relay(i - 1)

    e = HEAD**-0.5 * LOG2E
    heads_at_once = 2
    strip = heads_at_once * own
    for k in range(kv_heads):
        for j in range(n - 1):
            ok = me > j
            for via, b, _, which in relays:
                if b == j and k in which:
                    ok = ok & (me != via)
            @pl.when(ok)
            def _():
                send(k, j, lax.rem(me + 1, n), relay_sem.at[k]).wait_recv()
        if k >= kv_heads // 2:
            of = per // chunk_heads
            for i in range((k - kv_heads // 2) * of, (k - kv_heads // 2 + 1) * of):
                q_copy(i, 1 - side).wait_recv()
        keys = kv[order[k], :, :HEAD]
        values = jnp.concatenate([kv[order[k], :, HEAD:], jnp.ones((tokens, HEAD), kv.dtype)], axis=1)
        for u in range(per // heads_at_once):
            s = dot(q[ds((order[k] * (per // heads_at_once) + u) * strip, strip), :], keys, 1, 1)
            s = jnp.minimum(s, jnp.concatenate([cap[...]] * heads_at_once, axis=0))
            top = jnp.max(s, -1, keepdims=True)
            p = jnp.exp2((s - top) * e).astype(jnp.bfloat16)
            o = dot(p, values)
            o = (o[:, :HEAD] / o[:, HEAD:]).astype(jnp.bfloat16)
            for v in range(heads_at_once):
                h = u * heads_at_once + v
                seen[:, h * HEAD : (h + 1) * HEAD] = o[v * own : (v + 1) * own, :]
        for i in range(wo_per):
            at = k * wo_per + i
            wo_copy(at).wait()
            rows = pl.ds(i * wo_rows, wo_rows)
            for c in range(width // N_COLS):
                s = pl.ds(c * N_COLS, N_COLS)
                t = dot(seen[:, rows], wo[at % WO_SLOTS, :, s])
                if at == 0:
                    total[:, s] = t
                elif at < wo_chunks - 1:
                    total[:, s] += t
                else:
                    y[:, s] = (x[:, s].astype(jnp.float32) + (total[:, s] + t)).astype(y.dtype)
            if at == 0:
                relay(kv_heads - 1)
            if at + WO_SLOTS < wo_chunks:
                wo_copy(at + WO_SLOTS).start(priority=1)

    for i in range(PIECES):
        a_copy(i).wait_send()
    for i in range(q_chunks):
        q_copy(i, side).wait_send()
    for j, to, which in hops:
        @pl.when(me == j)
        def _():
            for k in which:
                send(k, j, to, send_sem.at[k, to]).wait_send()
    for via, j, to, which in relays:
        @pl.when(me == via)
        def _():
            for k in which:
                send(k, j, to, relay_sem.at[k]).wait_send()


def solution(mesh):
    n = mesh.shape["sp"]

    def step(x, gain, wq, wk, wv, wo):
        own, width = x.shape
        kv_heads, heads = wk.shape[1] // HEAD, wq.shape[1] // HEAD
        chunk = wk.shape[1]
        q_chunks = wq.shape[1] // (2 * chunk)
        tokens = n * own
        wo_rows = 512
        wo_chunks = wo.shape[0] // wo_rows
        anywhere = pl.BlockSpec(memory_space=pltpu.HBM)
        weights = sum(t.size for t in (wq, wk, wv, wo))
        vmem, f32, bf16, dma = pltpu.VMEM, jnp.float32, jnp.bfloat16, pltpu.SemaphoreType.DMA
        return pl.pallas_call(
            functools.partial(kernel, n),
            out_shape=jax.ShapeDtypeStruct(x.shape, x.dtype),
            in_specs=[anywhere] * 7,
            out_specs=pl.BlockSpec(memory_space=pltpu.VMEM),
            scratch_shapes=[
                vmem((own, width), bf16), vmem((width // LANES, LANES), bf16), vmem((own, 2 * HEAD), f32),
                vmem((2 * own, width), bf16), vmem((SLOTS, width, chunk), bf16), vmem((WO_SLOTS, wo_rows, width), bf16),
                vmem((heads * own, HEAD), bf16), vmem((heads // 2 * own, HEAD), bf16), vmem((kv_heads, tokens, 2 * HEAD), bf16),
                vmem((own, tokens), f32), vmem((own, heads // kv_heads * HEAD), bf16), vmem((own, width), f32),
                dma((3,)), dma((2 + q_chunks, 2)), dma((wo_chunks,)), dma((kv_heads, n)), dma((kv_heads,)), dma((kv_heads, n)),
                dma((PIECES,)), dma((PIECES,)), dma((q_chunks,)), dma((q_chunks,)),
            ],
            compiler_params=pltpu.CompilerParams(collective_id=0, has_side_effects=True, vmem_limit_bytes=52 * 2**20),
            cost_estimate=pl.CostEstimate(flops=2 * own * weights, bytes_accessed=2 * weights, transcendentals=heads * own * tokens),
        )(*(pltpu.with_memory_space_constraint(t, pltpu.HBM) for t in (x, gain.reshape(width // LANES, LANES), jnp.asarray(tables(tokens)), wq, wk, wv, wo)))

    rows, whole = P(("dp", "sp"), None), P(None, None)
    return jax.shard_map(
        step,
        mesh=mesh,
        in_specs=(rows, P(None), whole, whole, whole, whole),
        out_specs=rows,
        check_vma=False,
    )
```

```python
import functools

import jax
import jax.numpy as jnp
import numpy as np
from jax import lax
from jax.experimental import pallas as pl
from jax.experimental.pallas import tpu as pltpu
from jax.sharding import PartitionSpec as P

HEAD = 128
THETA = 10000
LOG2E = 1.4426950408889634
MESH = pl.DeviceIdType.MESH
LANES = 128
SLOTS = 4
WO_SLOTS = 6
PIECES = 4
N_COLS = 512
SENDS = [
    [(0, 0, 1), (0, 0, 3), (0, 1, 2), (0, 2, 3)],
    [(0, 0, 2), (1, 0, 3), (1, 2, 3)],
    [(1, 0, 1), (1, 1, 2)],
    [(2, 0, 3), (2, 1, 2), (1, 1, 3)],
    [(2, 0, 1), (1, 0, 2)],
    [(2, 2, 3), (3, 0, 3), (3, 0, 1), (2, 0, 2)],
    [(3, 1, 2), (3, 2, 3), (3, 0, 2), (3, 1, 3)],
    [],
]
RELAYS = {0: [(0, 2)], 1: [], 2: [], 3: [], 4: [(2, 2)]}
ORDER = [("s", 0), ("s", 1), ("w", 0), ("w", 1), ("w", 2), ("w", 3), ("p", 0), ("w", 4), ("w", 5), ("p", 1), ("w", 6), ("w", 7)]


def tables(tokens):
    half = HEAD // 2
    rate = np.float32(THETA) ** (-np.arange(half, dtype=np.float32) / np.float32(half))
    angle = (np.arange(tokens, dtype=np.float32)[:, None] * rate.astype(np.float32)).astype(np.float64)
    cos, sin = np.cos(angle).astype(np.float32), np.sin(angle).astype(np.float32)
    return np.concatenate([cos, cos, -sin, sin], -1)


def dot(a, b, ca=1, cb=0):
    return lax.dot_general(a, b, (((ca,), (cb,)), ((), ())), preferred_element_type=jnp.float32)


def kernel(n, x_hbm, gain_hbm, turn_hbm, wq_hbm, wk_hbm, wv_hbm, wo_hbm, y,
           x, gain, turn, a, w, wo, raw, q, q_out, kv, cap, seen, total,
           in_sem, kv_sem, w_sem, wo_sem, send_sem, relay_sem, recv_sem, a_send, a_recv, q_send, q_recv):
    me, group = lax.axis_index("sp"), lax.axis_index("dp")
    side = lax.rem(group, 2)
    partner = {"dp": group + 1 - 2 * side}
    own, width = x.shape
    kv_heads = kv.shape[0]
    heads = q.shape[0] // own
    per = heads // kv_heads
    chunk = w.shape[2]
    q_chunks = heads * HEAD // (2 * chunk)
    chunk_heads = chunk // HEAD
    chunks = 2 + q_chunks
    part = chunk // 2
    wo_rows = wo.shape[1]
    wo_chunks = heads * HEAD // wo_rows
    wo_per = wo_chunks // kv_heads
    tokens = n * own
    order = [lax.rem(kv_heads // 2 * side + k, kv_heads) for k in range(kv_heads)]

    def ds(at, size):
        return pl.ds(at if isinstance(at, int) else pl.multiple_of(at, size), size)

    mine = ds(me * own, own)

    place = pltpu.make_async_copy
    inputs = [
        place(x_hbm, x, in_sem.at[0]),
        place(gain_hbm, gain, in_sem.at[1]),
        place(turn_hbm.at[mine], turn, in_sem.at[2]),
    ]
    for c in inputs:
        c.start()

    def w_copy(i, half):
        at = ds((side * q_chunks + i - 2) * chunk + half * part, part)
        return place(wq_hbm.at[:, at], w.at[i % SLOTS, :, pl.ds(half * part, part)], w_sem.at[i, half])

    def kv_copy(i, k):
        return place((wk_hbm, wv_hbm)[i].at[:, ds(order[k] * HEAD, HEAD)], w.at[i, :, pl.ds(k * HEAD, HEAD)], kv_sem.at[i, k])

    def wo_copy(i):
        rows = ds(order[i // wo_per] * (wo_per * wo_rows) + i % wo_per * wo_rows, wo_rows)
        return place(wo_hbm.at[rows, :], wo.at[i % WO_SLOTS], wo_sem.at[i])

    def fetch(i):
        if i < chunks:
            for half in range(2):
                w_copy(i, half).start(priority=1)

    for k in range(kv_heads):
        for i in range(2):
            kv_copy(i, k).start(priority=1)
    for i in range(2, SLOTS):
        fetch(i)

    barrier = pltpu.get_barrier_semaphore()
    for step in range(1, n):
        pl.semaphore_signal(barrier, inc=1, device_id={"sp": lax.rem(me + step, n)}, device_id_type=MESH)
    pl.semaphore_signal(barrier, inc=1, device_id=partner, device_id_type=MESH)

    def block(k, j):
        return kv.at[order[k], ds(j * own, own), :]

    for j in range(1, n):
        for k in range(kv_heads):
            @pl.when(me < j)
            def _():
                block(k, j)[...] = jnp.zeros((own, 2 * HEAD), kv.dtype)
    place_q = me * own + lax.broadcasted_iota(jnp.int32, (own, tokens), 0)
    place_k = lax.broadcasted_iota(jnp.int32, (own, tokens), 1)
    cap[...] = jnp.where(place_q >= place_k, jnp.inf, -jnp.inf)

    for c in inputs:
        c.wait()
    cols = [slice(i * LANES, (i + 1) * LANES) for i in range(width // LANES)]
    square = jnp.zeros((own, LANES), jnp.float32)
    for s in cols:
        wide = x[:, s].astype(jnp.float32)
        square += wide * wide
    scale = lax.rsqrt(jnp.sum(square, -1, keepdims=True) * (1 / width) + 1e-6)

    def a_copy(i):
        tall = own // PIECES
        return pltpu.make_async_remote_copy(src_ref=a.at[pl.ds(i * tall, tall)], dst_ref=a.at[pl.ds(own + i * tall, tall)], send_sem=a_send.at[i],
                                            recv_sem=a_recv.at[i], device_id=partner, device_id_type=MESH)

    for i, s in enumerate(cols):
        a[:own, s] = (x[:, s].astype(jnp.float32) * scale * gain[i : i + 1, :].astype(jnp.float32)).astype(a.dtype)

    def turned(t):
        t = t.astype(jnp.bfloat16).astype(jnp.float32)
        return (t * turn[:, :HEAD] + pltpu.roll(t, HEAD // 2, 1) * turn[:, HEAD:]).astype(jnp.bfloat16)

    def send(k, j, to, sem):
        return pltpu.make_async_remote_copy(src_ref=block(k, j), dst_ref=block(k, j), send_sem=sem, recv_sem=recv_sem.at[k, j],
                                            device_id={"sp": to}, device_id_type=MESH)

    hops = [(j, j + 1, range(kv_heads)) for j in range(n - 1)] + [(0, 3, range(kv_heads)), (0, 2, range(kv_heads)), (1, 3, [1, 3])]
    relays = [(2, 1, 3, [0, 2])]

    def first_hop(*what):
        for j in range(n - 1):
            to = [(k, t) for k, f, t in what if f == j]
            if to:
                @pl.when(me == j)
                def _():
                    for k, t in to:
                        send(k, j, t, send_sem.at[k, t]).start()

    for k in range(kv_heads):
        for i in range(2):
            kv_copy(i, k).wait()
        s = pl.ds(k * HEAD, HEAD)
        kv[order[k], mine, :HEAD] = turned(dot(a[:own], w[0, :, s]))
        kv[order[k], mine, HEAD:] = dot(a[:own], w[1, :, s]).astype(jnp.bfloat16)
        if k == 0:
            pl.semaphore_wait(barrier, n)
            for i in range(PIECES):
                a_copy(i).start()
        first_hop(*SENDS[k])
    for i in range(SLOTS, SLOTS + 2):
        fetch(i)

    def relay(what):
        for via, j, to, which in relays:
            for k in which:
                if (k, via) in what:
                    @pl.when(me == via)
                    def _():
                        send(k, j, to, relay_sem.at[k]).wait_recv()
                        send(k, j, to, relay_sem.at[k]).start()

    def q_copy(i, whose):
        rows = pl.ds(i * chunk_heads * own, chunk_heads * own)
        there = ds((whose * q_chunks + i) * (chunk_heads * own), chunk_heads * own)
        return pltpu.make_async_remote_copy(src_ref=q_out.at[rows], dst_ref=q.at[there], send_sem=q_send.at[i], recv_sem=q_recv.at[i],
                                            device_id=partner, device_id_type=MESH)

    def turn_queries(i):
        for u in range(chunk_heads):
            s = slice(u * HEAD, (u + 1) * HEAD)
            h = i * chunk_heads + u
            q_out[h * own : (h + 1) * own, :] = turned(raw[i % 2, own:, s])
            q[ds((side * (heads // 2) + h) * own, own), :] = turned(raw[i % 2, :own, s])

    for i in range(q_chunks):
        for half in range(2):
            w_copy(2 + i, half).wait()
        if i == 0:
            raw[i % 2, :own] = dot(a[:own], w[(2 + i) % SLOTS]).astype(raw.dtype)
            for c in range(PIECES):
                a_copy(c).wait_recv()
            raw[i % 2, own:] = dot(a[own:], w[(2 + i) % SLOTS]).astype(raw.dtype)
        else:
            raw[i % 2] = dot(a[...], w[(2 + i) % SLOTS]).astype(raw.dtype)
        if i > 0:
            turn_queries(i - 1)
            q_copy(i - 1, side).start()
        for c in ([0, 1], [2], [3], [4, 5])[i]:
            wo_copy(c).start(priority=1)
        relay(RELAYS[i])
        first_hop(*SENDS[kv_heads + i])

    e = HEAD**-0.5 * LOG2E
    heads_at_once = 2
    strip = heads_at_once * own
    strips = wo_rows // (heads_at_once * HEAD)

    def output(j, c):
        s = pl.ds(c * N_COLS, N_COLS)
        t = dot(seen[j % 2], wo[j % WO_SLOTS, :, s])
        if j == 0:
            total[:, s] = t
        elif j < wo_chunks - 1:
            total[:, s] += t
        else:
            y[:, s] = (x[:, s].astype(jnp.float32) + (total[:, s] + t)).astype(y.dtype)

    pieces = width // N_COLS
    for j in range(wo_chunks):
        k = j // wo_per
        if j % wo_per == 0:
            for b in range(n - 1):
                ok = me > b
                for via, of, _, which in relays:
                    if of == b and k in which:
                        ok = ok & (me != via)
                @pl.when(ok)
                def _():
                    send(k, b, lax.rem(me + 1, n), relay_sem.at[k]).wait_recv()
            if k >= kv_heads // 2:
                of = per // chunk_heads
                for i in range((k - kv_heads // 2) * of, (k - kv_heads // 2 + 1) * of):
                    q_copy(i, 1 - side).wait_recv()
        if j > 0:
            wo_copy(j - 1).wait()
        else:
            turn_queries(q_chunks - 1)
        keys = kv[order[k], :, :HEAD]
        values = jnp.concatenate([kv[order[k], :, HEAD:], jnp.ones((tokens, HEAD), kv.dtype)], axis=1)
        scores = {}
        for kind, u in ORDER:
            if kind == "s":
                at = (order[k] * wo_per + j % wo_per) * strips + u
                scores[u] = dot(q[ds(at * strip, strip), :], keys, 1, 1)
            elif kind == "w":
                if j > 0:
                    output(j - 1, u)
            else:
                s = jnp.minimum(scores[u], jnp.concatenate([cap[...]] * heads_at_once, axis=0))
                top = jnp.max(s, -1, keepdims=True)
                p = jnp.exp2((s - top) * e).astype(jnp.bfloat16)
                o = dot(p, values)
                o = (o[:, :HEAD] / o[:, HEAD:]).astype(jnp.bfloat16)
                for v in range(heads_at_once):
                    h = u * heads_at_once + v
                    seen[j % 2, :, h * HEAD : (h + 1) * HEAD] = o[v * own : (v + 1) * own, :]
        if j == 0:
            q_copy(q_chunks - 1, side).start()
        elif j - 1 + WO_SLOTS < wo_chunks:
            wo_copy(j - 1 + WO_SLOTS).start(priority=1)
        relay(RELAYS.get(q_chunks + j, []))
    wo_copy(wo_chunks - 1).wait()
    for c in range(pieces):
        output(wo_chunks - 1, c)

    for i in range(PIECES):
        a_copy(i).wait_send()
    for i in range(q_chunks):
        q_copy(i, side).wait_send()
    for j, to, which in hops:
        @pl.when(me == j)
        def _():
            for k in which:
                send(k, j, to, send_sem.at[k, to]).wait_send()
    for via, j, to, which in relays:
        @pl.when(me == via)
        def _():
            for k in which:
                send(k, j, to, relay_sem.at[k]).wait_send()


def solution(mesh):
    n = mesh.shape["sp"]

    def step(x, gain, wq, wk, wv, wo):
        own, width = x.shape
        kv_heads, heads = wk.shape[1] // HEAD, wq.shape[1] // HEAD
        chunk = wk.shape[1]
        q_chunks = wq.shape[1] // (2 * chunk)
        tokens = n * own
        wo_rows = 512
        wo_chunks = wo.shape[0] // wo_rows
        anywhere = pl.BlockSpec(memory_space=pltpu.HBM)
        weights = sum(t.size for t in (wq, wk, wv, wo))
        vmem, f32, bf16, dma = pltpu.VMEM, jnp.float32, jnp.bfloat16, pltpu.SemaphoreType.DMA
        return pl.pallas_call(
            functools.partial(kernel, n),
            out_shape=jax.ShapeDtypeStruct(x.shape, x.dtype),
            in_specs=[anywhere] * 7,
            out_specs=pl.BlockSpec(memory_space=pltpu.VMEM),
            scratch_shapes=[
                vmem((own, width), bf16), vmem((width // LANES, LANES), bf16), vmem((own, 2 * HEAD), f32),
                vmem((2 * own, width), bf16), vmem((SLOTS, width, chunk), bf16), vmem((WO_SLOTS, wo_rows, width), bf16),
                vmem((2, 2 * own, chunk), bf16),
                vmem((heads * own, HEAD), bf16), vmem((heads // 2 * own, HEAD), bf16), vmem((kv_heads, tokens, 2 * HEAD), bf16),
                vmem((own, tokens), f32), vmem((2, own, wo_rows), bf16), vmem((own, width), f32),
                dma((3,)), dma((2, kv_heads)), dma((2 + q_chunks, 2)), dma((wo_chunks,)), dma((kv_heads, n)), dma((kv_heads,)), dma((kv_heads, n)),
                dma((PIECES,)), dma((PIECES,)), dma((q_chunks,)), dma((q_chunks,)),
            ],
            compiler_params=pltpu.CompilerParams(collective_id=0, has_side_effects=True, vmem_limit_bytes=52 * 2**20),
            cost_estimate=pl.CostEstimate(flops=2 * own * weights, bytes_accessed=2 * weights, transcendentals=heads * own * tokens),
        )(*(pltpu.with_memory_space_constraint(t, pltpu.HBM) for t in (x, gain.reshape(width // LANES, LANES), jnp.asarray(tables(tokens)), wq, wk, wv, wo)))

    rows, whole = P(("dp", "sp"), None), P(None, None)
    return jax.shard_map(
        step,
        mesh=mesh,
        in_specs=(rows, P(None), whole, whole, whole, whole),
        out_specs=rows,
        check_vma=False,
    )
```

```python
import functools

import jax
import jax.numpy as jnp
import numpy as np
from jax import lax
from jax.experimental import pallas as pl
from jax.experimental.pallas import tpu as pltpu
from jax.sharding import PartitionSpec as P

HEAD = 128
THETA = 10000
LOG2E = 1.4426950408889634
MESH = pl.DeviceIdType.MESH
LANES = 128
SLOTS = 5
WO_SLOTS = 5
PIECES = 4
N_COLS = 512
SENDS = [
    [(0, 0, 1), (0, 0, 3), (0, 1, 2), (0, 2, 3)],
    [(0, 0, 2), (1, 0, 3), (1, 2, 3)],
    [(1, 0, 1), (1, 1, 2)],
    [(2, 0, 3), (2, 1, 2), (1, 1, 3)],
    [(2, 0, 1), (1, 0, 2)],
    [(2, 2, 3), (3, 0, 3), (3, 0, 1), (2, 0, 2)],
    [(3, 1, 2), (3, 2, 3), (3, 0, 2), (3, 1, 3)],
    [],
]
RELAYS = {0: [(0, 2)], 1: [], 2: [], 3: [], 4: [(2, 2)]}
ORDER = [("s", 0), ("w", 0), ("w", 1), ("s", 1), ("w", 2), ("w", 3), ("p", 0), ("w", 4), ("w", 5), ("p", 1), ("w", 6), ("w", 7)]


def tables(tokens):
    half = HEAD // 2
    rate = np.float32(THETA) ** (-np.arange(half, dtype=np.float32) / np.float32(half))
    angle = (np.arange(tokens, dtype=np.float32)[:, None] * rate.astype(np.float32)).astype(np.float64)
    cos, sin = np.cos(angle).astype(np.float32), np.sin(angle).astype(np.float32)
    return np.concatenate([cos, cos, -sin, sin], -1)


def dot(a, b, ca=1, cb=0):
    return lax.dot_general(a, b, (((ca,), (cb,)), ((), ())), preferred_element_type=jnp.float32)


def kernel(n, x_hbm, gain_hbm, turn_hbm, wq_hbm, wk_hbm, wv_hbm, wo_hbm, y,
           x, gain, turn, a, w, wo, raw, q, q_out, kv, cap, seen, total,
           in_sem, kv_sem, w_sem, wo_sem, send_sem, relay_sem, recv_sem, a_send, a_recv, q_send, q_recv):
    me, group = lax.axis_index("sp"), lax.axis_index("dp")
    side = lax.rem(group, 2)
    partner = {"dp": group + 1 - 2 * side}
    own, width = x.shape
    kv_heads = kv.shape[0]
    heads = q.shape[0] // own
    per = heads // kv_heads
    chunk = w.shape[2]
    q_chunks = heads * HEAD // (2 * chunk)
    chunk_heads = chunk // HEAD
    chunks = 2 + q_chunks
    part = chunk // 2
    wo_rows = wo.shape[1]
    wo_chunks = heads * HEAD // wo_rows
    wo_per = wo_chunks // kv_heads
    tokens = n * own
    order = [lax.rem(kv_heads // 2 * side + k, kv_heads) for k in range(kv_heads)]

    def ds(at, size):
        return pl.ds(at if isinstance(at, int) else pl.multiple_of(at, size), size)

    mine = ds(me * own, own)

    place = pltpu.make_async_copy
    inputs = [
        place(x_hbm, x, in_sem.at[0]),
        place(gain_hbm, gain, in_sem.at[1]),
        place(turn_hbm.at[mine], turn, in_sem.at[2]),
    ]
    for c in inputs:
        c.start()

    def w_copy(i, half):
        at = ds((side * q_chunks + i - 2) * chunk + half * part, part)
        return place(wq_hbm.at[:, at], w.at[i % SLOTS, :, pl.ds(half * part, part)], w_sem.at[i, half])

    def kv_copy(i, k):
        return place((wk_hbm, wv_hbm)[i].at[:, ds(order[k] * HEAD, HEAD)], w.at[i, :, pl.ds(k * HEAD, HEAD)], kv_sem.at[i, k])

    def wo_copy(i):
        rows = ds(order[i // wo_per] * (wo_per * wo_rows) + i % wo_per * wo_rows, wo_rows)
        return place(wo_hbm.at[rows, :], wo.at[i % WO_SLOTS], wo_sem.at[i])

    def fetch(i):
        if i < chunks:
            for half in range(2):
                w_copy(i, half).start(priority=1)

    for k in range(kv_heads):
        for i in range(2):
            kv_copy(i, k).start(priority=1)
    for i in range(2, SLOTS):
        fetch(i)

    barrier = pltpu.get_barrier_semaphore()
    for step in range(1, n):
        pl.semaphore_signal(barrier, inc=1, device_id={"sp": lax.rem(me + step, n)}, device_id_type=MESH)
    pl.semaphore_signal(barrier, inc=1, device_id=partner, device_id_type=MESH)

    def block(k, j):
        return kv.at[order[k], ds(j * own, own), :]

    for j in range(1, n):
        for k in range(kv_heads):
            @pl.when(me < j)
            def _():
                block(k, j)[...] = jnp.zeros((own, 2 * HEAD), kv.dtype)
    place_q = me * own + lax.broadcasted_iota(jnp.int32, (own, tokens), 0)
    place_k = lax.broadcasted_iota(jnp.int32, (own, tokens), 1)
    cap[...] = jnp.where(place_q >= place_k, jnp.inf, -jnp.inf)

    for c in inputs:
        c.wait()
    cols = [slice(i * LANES, (i + 1) * LANES) for i in range(width // LANES)]
    square = jnp.zeros((own, LANES), jnp.float32)
    for s in cols:
        wide = x[:, s].astype(jnp.float32)
        square += wide * wide
    scale = lax.rsqrt(jnp.sum(square, -1, keepdims=True) * (1 / width) + 1e-6)

    def a_copy(i):
        tall = own // PIECES
        return pltpu.make_async_remote_copy(src_ref=a.at[pl.ds(i * tall, tall)], dst_ref=a.at[pl.ds(own + i * tall, tall)], send_sem=a_send.at[i],
                                            recv_sem=a_recv.at[i], device_id=partner, device_id_type=MESH)

    for i, s in enumerate(cols):
        a[:own, s] = (x[:, s].astype(jnp.float32) * scale * gain[i : i + 1, :].astype(jnp.float32)).astype(a.dtype)

    def turned(t):
        t = t.astype(jnp.bfloat16).astype(jnp.float32)
        return (t * turn[:, :HEAD] + pltpu.roll(t, HEAD // 2, 1) * turn[:, HEAD:]).astype(jnp.bfloat16)

    def send(k, j, to, sem):
        return pltpu.make_async_remote_copy(src_ref=block(k, j), dst_ref=block(k, j), send_sem=sem, recv_sem=recv_sem.at[k, j],
                                            device_id={"sp": to}, device_id_type=MESH)

    hops = [(j, j + 1, range(kv_heads)) for j in range(n - 1)] + [(0, 3, range(kv_heads)), (0, 2, range(kv_heads)), (1, 3, [1, 3])]
    relays = [(2, 1, 3, [0, 2])]

    def first_hop(*what):
        for j in range(n - 1):
            to = [(k, t) for k, f, t in what if f == j]
            if to:
                @pl.when(me == j)
                def _():
                    for k, t in to:
                        send(k, j, t, send_sem.at[k, t]).start()

    for k in range(kv_heads):
        for i in range(2):
            kv_copy(i, k).wait()
        s = pl.ds(k * HEAD, HEAD)
        kv[order[k], mine, :HEAD] = turned(dot(a[:own], w[0, :, s]))
        kv[order[k], mine, HEAD:] = dot(a[:own], w[1, :, s]).astype(jnp.bfloat16)
        if k == 0:
            pl.semaphore_wait(barrier, n)
            for i in range(PIECES):
                a_copy(i).start()
        first_hop(*SENDS[k])
    for i in range(SLOTS, SLOTS + 2):
        fetch(i)

    def relay(what):
        for via, j, to, which in relays:
            for k in which:
                if (k, via) in what:
                    @pl.when(me == via)
                    def _():
                        send(k, j, to, relay_sem.at[k]).wait_recv()
                        send(k, j, to, relay_sem.at[k]).start()

    def q_copy(i, whose):
        rows = pl.ds(i * chunk_heads * own, chunk_heads * own)
        there = ds((whose * q_chunks + i) * (chunk_heads * own), chunk_heads * own)
        return pltpu.make_async_remote_copy(src_ref=q_out.at[rows], dst_ref=q.at[there], send_sem=q_send.at[i], recv_sem=q_recv.at[i],
                                            device_id=partner, device_id_type=MESH)

    def turn_queries(i):
        for u in range(chunk_heads):
            s = slice(u * HEAD, (u + 1) * HEAD)
            h = i * chunk_heads + u
            q_out[h * own : (h + 1) * own, :] = turned(raw[i % 2, own:, s])
            q[ds((side * (heads // 2) + h) * own, own), :] = turned(raw[i % 2, :own, s])

    for i in range(q_chunks):
        for half in range(2):
            w_copy(2 + i, half).wait()
        if i == 0:
            raw[i % 2, :own] = dot(a[:own], w[(2 + i) % SLOTS]).astype(raw.dtype)
            for c in range(PIECES):
                a_copy(c).wait_recv()
            raw[i % 2, own:] = dot(a[own:], w[(2 + i) % SLOTS]).astype(raw.dtype)
        else:
            raw[i % 2] = dot(a[...], w[(2 + i) % SLOTS]).astype(raw.dtype)
        if i > 0:
            turn_queries(i - 1)
            q_copy(i - 1, side).start()
        for c in ([0, 1], [2], [3], [4])[i]:
            wo_copy(c).start(priority=1)
        relay(RELAYS[i])
        first_hop(*SENDS[kv_heads + i])

    e = HEAD**-0.5 * LOG2E
    heads_at_once = 2
    strip = heads_at_once * own
    strips = wo_rows // (heads_at_once * HEAD)

    def output(j, c):
        s = pl.ds(c * N_COLS, N_COLS)
        t = dot(seen[j % 2], wo[j % WO_SLOTS, :, s])
        if j == 0:
            total[:, s] = t
        elif j < wo_chunks - 1:
            total[:, s] += t
        else:
            y[:, s] = (x[:, s].astype(jnp.float32) + (total[:, s] + t)).astype(y.dtype)

    pieces = width // N_COLS
    def attend(seen_blocks):
        in_view = seen_blocks * own
        for j in range(wo_chunks):
            k = j // wo_per
            if j % wo_per == 0:
                for b in range(seen_blocks - 1):
                    ok = me > b
                    for via, of, _, which in relays:
                        if of == b and k in which:
                            ok = ok & (me != via)
                    @pl.when(ok)
                    def _():
                        send(k, b, lax.rem(me + 1, n), relay_sem.at[k]).wait_recv()
                if k >= kv_heads // 2:
                    of = per // chunk_heads
                    for i in range((k - kv_heads // 2) * of, (k - kv_heads // 2 + 1) * of):
                        q_copy(i, 1 - side).wait_recv()
            if j > 0:
                wo_copy(j - 1).wait()
            else:
                turn_queries(q_chunks - 1)
            keys = kv[order[k], :in_view, :HEAD]
            values = jnp.concatenate([kv[order[k], :in_view, HEAD:], jnp.ones((in_view, HEAD), kv.dtype)], axis=1)
            scores = {}
            for kind, u in ORDER:
                if kind == "s":
                    at = (order[k] * wo_per + j % wo_per) * strips + u
                    scores[u] = dot(q[ds(at * strip, strip), :], keys, 1, 1)
                elif kind == "w":
                    if j > 0:
                        output(j - 1, u)
                else:
                    s = jnp.minimum(scores[u], jnp.concatenate([cap[:, :in_view]] * heads_at_once, axis=0))
                    top = jnp.max(s, -1, keepdims=True)
                    p = jnp.exp2((s - top) * e).astype(jnp.bfloat16)
                    o = dot(p, values)
                    o = (o[:, :HEAD] / o[:, HEAD:]).astype(jnp.bfloat16)
                    for v in range(heads_at_once):
                        h = u * heads_at_once + v
                        seen[j % 2, :, h * HEAD : (h + 1) * HEAD] = o[v * own : (v + 1) * own, :]
            if j == 0:
                q_copy(q_chunks - 1, side).start()
            elif j - 1 + WO_SLOTS < wo_chunks:
                wo_copy(j - 1 + WO_SLOTS).start(priority=1)
            relay(RELAYS.get(q_chunks + j, []))

    pl.when(me == 0)(lambda: attend(1))
    pl.when(me != 0)(lambda: attend(n))
    wo_copy(wo_chunks - 1).wait()
    for c in range(pieces):
        output(wo_chunks - 1, c)

    for i in range(PIECES):
        a_copy(i).wait_send()
    for i in range(q_chunks):
        q_copy(i, side).wait_send()
    for j, to, which in hops:
        @pl.when(me == j)
        def _():
            for k in which:
                send(k, j, to, send_sem.at[k, to]).wait_send()
    for via, j, to, which in relays:
        @pl.when(me == via)
        def _():
            for k in which:
                send(k, j, to, relay_sem.at[k]).wait_send()


def solution(mesh):
    n = mesh.shape["sp"]

    def step(x, gain, wq, wk, wv, wo):
        own, width = x.shape
        kv_heads, heads = wk.shape[1] // HEAD, wq.shape[1] // HEAD
        chunk = wk.shape[1]
        q_chunks = wq.shape[1] // (2 * chunk)
        tokens = n * own
        wo_rows = 512
        wo_chunks = wo.shape[0] // wo_rows
        anywhere = pl.BlockSpec(memory_space=pltpu.HBM)
        weights = sum(t.size for t in (wq, wk, wv, wo))
        vmem, f32, bf16, dma = pltpu.VMEM, jnp.float32, jnp.bfloat16, pltpu.SemaphoreType.DMA
        return pl.pallas_call(
            functools.partial(kernel, n),
            out_shape=jax.ShapeDtypeStruct(x.shape, x.dtype),
            in_specs=[anywhere] * 7,
            out_specs=pl.BlockSpec(memory_space=pltpu.VMEM),
            scratch_shapes=[
                vmem((own, width), bf16), vmem((width // LANES, LANES), bf16), vmem((own, 2 * HEAD), f32),
                vmem((2 * own, width), bf16), vmem((SLOTS, width, chunk), bf16), vmem((WO_SLOTS, wo_rows, width), bf16),
                vmem((2, 2 * own, chunk), bf16),
                vmem((heads * own, HEAD), bf16), vmem((heads // 2 * own, HEAD), bf16), vmem((kv_heads, tokens, 2 * HEAD), bf16),
                vmem((own, tokens), f32), vmem((2, own, wo_rows), bf16), vmem((own, width), f32),
                dma((3,)), dma((2, kv_heads)), dma((2 + q_chunks, 2)), dma((wo_chunks,)), dma((kv_heads, n)), dma((kv_heads,)), dma((kv_heads, n)),
                dma((PIECES,)), dma((PIECES,)), dma((q_chunks,)), dma((q_chunks,)),
            ],
            compiler_params=pltpu.CompilerParams(collective_id=0, has_side_effects=True, vmem_limit_bytes=52 * 2**20),
            cost_estimate=pl.CostEstimate(flops=2 * own * weights, bytes_accessed=2 * weights, transcendentals=heads * own * tokens),
        )(*(pltpu.with_memory_space_constraint(t, pltpu.HBM) for t in (x, gain.reshape(width // LANES, LANES), jnp.asarray(tables(tokens)), wq, wk, wv, wo)))

    rows, whole = P(("dp", "sp"), None), P(None, None)
    return jax.shard_map(
        step,
        mesh=mesh,
        in_specs=(rows, P(None), whole, whole, whole, whole),
        out_specs=rows,
        check_vma=False,
    )
```

```python
import functools

import jax
import jax.numpy as jnp
import numpy as np
from jax import lax
from jax.experimental import pallas as pl
from jax.experimental.pallas import tpu as pltpu
from jax.sharding import PartitionSpec as P

HEAD = 128
THETA = 10000
LOG2E = 1.4426950408889634
MESH = pl.DeviceIdType.MESH
LANES = 128
SLOTS = 5
WO_SLOTS = 5
PIECES = 1
N_COLS = 512
SENDS = [
    [(0, 0, 1), (0, 0, 3), (0, 1, 2), (0, 2, 3)],
    [(0, 0, 2), (1, 0, 3), (1, 2, 3)],
    [(1, 0, 1), (1, 1, 2)],
    [(2, 0, 3), (2, 1, 2), (1, 1, 3)],
    [(2, 0, 1), (1, 0, 2)],
    [(2, 2, 3), (3, 0, 3), (3, 0, 1), (2, 0, 2)],
    [(3, 1, 2), (3, 2, 3), (3, 0, 2), (3, 1, 3)],
    [],
]
RELAYS = {0: [(0, 2)], 1: [], 2: [], 3: [], 4: [(2, 2)]}
ORDER = [("s", 0), ("w", 0), ("w", 1), ("s", 1), ("w", 2), ("w", 3), ("p", 0), ("w", 4), ("w", 5), ("p", 1), ("w", 6), ("w", 7)]


def tables(tokens):
    half = HEAD // 2
    rate = np.float32(THETA) ** (-np.arange(half, dtype=np.float32) / np.float32(half))
    angle = (np.arange(tokens, dtype=np.float32)[:, None] * rate.astype(np.float32)).astype(np.float64)
    cos, sin = np.cos(angle).astype(np.float32), np.sin(angle).astype(np.float32)
    return np.concatenate([cos, cos, -sin, sin], -1)


def dot(a, b, ca=1, cb=0):
    return lax.dot_general(a, b, (((ca,), (cb,)), ((), ())), preferred_element_type=jnp.float32)


def kernel(n, x_hbm, gain_hbm, turn_hbm, wq_hbm, wk_hbm, wv_hbm, wo_hbm, y,
           x, gain, turn, a, w, wo, raw, q, q_out, kv, cap, seen, total,
           recv_sem, a_recv, q_recv, in_sem, kv_sem, w_sem, wo_sem, send_sem, relay_sem, a_send, q_send):
    me, group = lax.axis_index("sp"), lax.axis_index("dp")
    side = lax.rem(group, 2)
    partner = {"dp": group + 1 - 2 * side}
    own, width = x.shape
    kv_heads = kv.shape[0]
    heads = q.shape[0] // own
    per = heads // kv_heads
    chunk = w.shape[2]
    q_chunks = heads * HEAD // (2 * chunk)
    chunk_heads = chunk // HEAD
    chunks = 2 + q_chunks
    part = chunk // 2
    wo_rows = wo.shape[1]
    wo_chunks = heads * HEAD // wo_rows
    wo_per = wo_chunks // kv_heads
    tokens = n * own
    order = [lax.rem(kv_heads // 2 * side + k, kv_heads) for k in range(kv_heads)]

    def ds(at, size):
        return pl.ds(at if isinstance(at, int) else pl.multiple_of(at, size), size)

    mine = ds(me * own, own)

    place = pltpu.make_async_copy
    inputs = [
        place(x_hbm, x, in_sem.at[0]),
        place(gain_hbm, gain, in_sem.at[1]),
        place(turn_hbm.at[mine], turn, in_sem.at[2]),
    ]
    for c in inputs:
        c.start()

    def w_copy(i, half):
        at = ds((side * q_chunks + i - 2) * chunk + half * part, part)
        return place(wq_hbm.at[:, at], w.at[i % SLOTS, :, pl.ds(half * part, part)], w_sem.at[i, half])

    def kv_copy(i, k):
        return place((wk_hbm, wv_hbm)[i].at[:, ds(order[k] * HEAD, HEAD)], w.at[i, :, pl.ds(k * HEAD, HEAD)], kv_sem.at[i, k])

    def wo_copy(i):
        rows = ds(order[i // wo_per] * (wo_per * wo_rows) + i % wo_per * wo_rows, wo_rows)
        return place(wo_hbm.at[rows, :], wo.at[i % WO_SLOTS], wo_sem.at[i])

    def fetch(i):
        if i < chunks:
            for half in range(2):
                w_copy(i, half).start(priority=1)

    for k in range(kv_heads):
        for i in range(2):
            kv_copy(i, k).start(priority=1)
    for i in range(2, SLOTS):
        fetch(i)

    barrier = pltpu.get_barrier_semaphore()
    for step in range(1, n):
        pl.semaphore_signal(barrier, inc=1, device_id={"sp": lax.rem(me + step, n)}, device_id_type=MESH)
    pl.semaphore_signal(barrier, inc=1, device_id=partner, device_id_type=MESH)

    def block(k, j):
        return kv.at[order[k], ds(j * own, own), :]

    for j in range(1, n):
        for k in range(kv_heads):
            @pl.when(me < j)
            def _():
                block(k, j)[...] = jnp.zeros((own, 2 * HEAD), kv.dtype)
    place_q = me * own + lax.broadcasted_iota(jnp.int32, (own, tokens), 0)
    place_k = lax.broadcasted_iota(jnp.int32, (own, tokens), 1)
    cap[...] = jnp.where(place_q >= place_k, jnp.inf, -jnp.inf)

    for c in inputs:
        c.wait()
    cols = [slice(i * LANES, (i + 1) * LANES) for i in range(width // LANES)]
    square = jnp.zeros((own, LANES), jnp.float32)
    for s in cols:
        wide = x[:, s].astype(jnp.float32)
        square += wide * wide
    scale = lax.rsqrt(jnp.sum(square, -1, keepdims=True) * (1 / width) + 1e-6)

    def a_copy(i):
        tall = own // PIECES
        return pltpu.make_async_remote_copy(src_ref=a.at[pl.ds(i * tall, tall)], dst_ref=a.at[pl.ds(own + i * tall, tall)], send_sem=a_send.at[i],
                                            recv_sem=a_recv.at[i], device_id=partner, device_id_type=MESH)

    for i, s in enumerate(cols):
        a[:own, s] = (x[:, s].astype(jnp.float32) * scale * gain[i : i + 1, :].astype(jnp.float32)).astype(a.dtype)

    def turned(t):
        t = t.astype(jnp.bfloat16).astype(jnp.float32)
        return (t * turn[:, :HEAD] + pltpu.roll(t, HEAD // 2, 1) * turn[:, HEAD:]).astype(jnp.bfloat16)

    def send(k, j, to, sem):
        return pltpu.make_async_remote_copy(src_ref=block(k, j), dst_ref=block(k, j), send_sem=sem, recv_sem=recv_sem.at[k, j],
                                            device_id={"sp": to}, device_id_type=MESH)

    hops = [(j, j + 1, range(kv_heads)) for j in range(n - 1)] + [(0, 3, range(kv_heads)), (0, 2, range(kv_heads)), (1, 3, [1, 3])]
    relays = [(2, 1, 3, [0, 2])]

    def first_hop(*what):
        for j in range(n - 1):
            to = [(k, t) for k, f, t in what if f == j]
            if to:
                @pl.when(me == j)
                def _():
                    for k, t in to:
                        send(k, j, t, send_sem.at[k, t]).start()

    for k in range(kv_heads):
        for i in range(2):
            kv_copy(i, k).wait()
        s = pl.ds(k * HEAD, HEAD)
        kv[order[k], mine, :HEAD] = turned(dot(a[:own], w[0, :, s]))
        kv[order[k], mine, HEAD:] = dot(a[:own], w[1, :, s]).astype(jnp.bfloat16)
        if k == 0:
            pl.semaphore_wait(barrier, n)
            for i in range(PIECES):
                a_copy(i).start()
        first_hop(*SENDS[k])
    for i in range(SLOTS, SLOTS + 2):
        fetch(i)

    def relay(what):
        for via, j, to, which in relays:
            for k in which:
                if (k, via) in what:
                    @pl.when(me == via)
                    def _():
                        send(k, j, to, relay_sem.at[k]).wait_recv()
                        send(k, j, to, relay_sem.at[k]).start()

    def q_copy(i, whose):
        rows = pl.ds(i * chunk_heads * own, chunk_heads * own)
        there = ds((whose * q_chunks + i) * (chunk_heads * own), chunk_heads * own)
        return pltpu.make_async_remote_copy(src_ref=q_out.at[rows], dst_ref=q.at[there], send_sem=q_send.at[i], recv_sem=q_recv.at[i],
                                            device_id=partner, device_id_type=MESH)

    def turn_queries(i):
        for u in range(chunk_heads):
            s = slice(u * HEAD, (u + 1) * HEAD)
            h = i * chunk_heads + u
            q_out[h * own : (h + 1) * own, :] = turned(raw[i % 2, own:, s])
            q[ds((side * (heads // 2) + h) * own, own), :] = turned(raw[i % 2, :own, s])

    for i in range(q_chunks):
        for half in range(2):
            w_copy(2 + i, half).wait()
        if i == 0:
            raw[i % 2, :own] = dot(a[:own], w[(2 + i) % SLOTS]).astype(raw.dtype)
            for c in range(PIECES):
                a_copy(c).wait_recv()
            raw[i % 2, own:] = dot(a[own:], w[(2 + i) % SLOTS]).astype(raw.dtype)
        else:
            raw[i % 2] = dot(a[...], w[(2 + i) % SLOTS]).astype(raw.dtype)
        if i > 0:
            turn_queries(i - 1)
            q_copy(i - 1, side).start()
        for c in ([0, 1], [2], [3], [4])[i]:
            wo_copy(c).start(priority=1)
        relay(RELAYS[i])
        first_hop(*SENDS[kv_heads + i])

    e = HEAD**-0.5 * LOG2E
    heads_at_once = 2
    strip = heads_at_once * own
    strips = wo_rows // (heads_at_once * HEAD)

    def output(j, c):
        s = pl.ds(c * N_COLS, N_COLS)
        t = dot(seen[j % 2], wo[j % WO_SLOTS, :, s])
        if j == 0:
            total[:, s] = t
        elif j < wo_chunks - 1:
            total[:, s] += t
        else:
            y[:, s] = (x[:, s].astype(jnp.float32) + (total[:, s] + t)).astype(y.dtype)

    pieces = width // N_COLS
    def attend(seen_blocks):
        in_view = seen_blocks * own
        for j in range(wo_chunks):
            k = j // wo_per
            if j % wo_per == 0:
                for b in range(seen_blocks - 1):
                    ok = me > b
                    for via, of, _, which in relays:
                        if of == b and k in which:
                            ok = ok & (me != via)
                    @pl.when(ok)
                    def _():
                        send(k, b, lax.rem(me + 1, n), relay_sem.at[k]).wait_recv()
                if k >= kv_heads // 2:
                    of = per // chunk_heads
                    for i in range((k - kv_heads // 2) * of, (k - kv_heads // 2 + 1) * of):
                        q_copy(i, 1 - side).wait_recv()
            if j > 0:
                wo_copy(j - 1).wait()
            else:
                turn_queries(q_chunks - 1)
            keys = kv[order[k], :in_view, :HEAD]
            values = jnp.concatenate([kv[order[k], :in_view, HEAD:], jnp.ones((in_view, HEAD), kv.dtype)], axis=1)
            scores = {}
            for kind, u in ORDER:
                if kind == "s":
                    at = (order[k] * wo_per + j % wo_per) * strips + u
                    scores[u] = dot(q[ds(at * strip, strip), :], keys, 1, 1)
                elif kind == "w":
                    if j > 0:
                        output(j - 1, u)
                else:
                    s = jnp.minimum(scores[u], jnp.concatenate([cap[:, :in_view]] * heads_at_once, axis=0))
                    top = jnp.max(s, -1, keepdims=True)
                    p = jnp.exp2((s - top) * e).astype(jnp.bfloat16)
                    o = dot(p, values)
                    o = (o[:, :HEAD] / o[:, HEAD:]).astype(jnp.bfloat16)
                    for v in range(heads_at_once):
                        h = u * heads_at_once + v
                        seen[j % 2, :, h * HEAD : (h + 1) * HEAD] = o[v * own : (v + 1) * own, :]
            if j == 0:
                q_copy(q_chunks - 1, side).start()
            elif j - 1 + WO_SLOTS < wo_chunks:
                wo_copy(j - 1 + WO_SLOTS).start(priority=1)
            relay(RELAYS.get(q_chunks + j, []))

    pl.when(me == 0)(lambda: attend(1))
    pl.when(me != 0)(lambda: attend(n))
    wo_copy(wo_chunks - 1).wait()
    for c in range(pieces):
        output(wo_chunks - 1, c)

    for i in range(PIECES):
        a_copy(i).wait_send()
    for i in range(q_chunks):
        q_copy(i, side).wait_send()
    for j, to, which in hops:
        @pl.when(me == j)
        def _():
            for k in which:
                send(k, j, to, send_sem.at[k, to]).wait_send()
    for via, j, to, which in relays:
        @pl.when(me == via)
        def _():
            for k in which:
                send(k, j, to, relay_sem.at[k]).wait_send()


def scoped(n, semaphores, *refs):
    pl.run_scoped(lambda *local: kernel(n, *refs, *local), *semaphores)


def solution(mesh):
    n = mesh.shape["sp"]

    def step(x, gain, wq, wk, wv, wo):
        own, width = x.shape
        kv_heads, heads = wk.shape[1] // HEAD, wq.shape[1] // HEAD
        chunk = wk.shape[1]
        q_chunks = wq.shape[1] // (2 * chunk)
        tokens = n * own
        wo_rows = 512
        wo_chunks = wo.shape[0] // wo_rows
        anywhere = pl.BlockSpec(memory_space=pltpu.HBM)
        weights = sum(t.size for t in (wq, wk, wv, wo))
        vmem, f32, bf16, dma = pltpu.VMEM, jnp.float32, jnp.bfloat16, pltpu.SemaphoreType.DMA
        local = [dma((3,)), dma((2, kv_heads)), dma((2 + q_chunks, 2)), dma((wo_chunks,)), dma((kv_heads, n)), dma((kv_heads,)), dma((PIECES,)),
                 dma((q_chunks,))]
        return pl.pallas_call(
            functools.partial(scoped, n, local),
            out_shape=jax.ShapeDtypeStruct(x.shape, x.dtype),
            in_specs=[anywhere] * 7,
            out_specs=pl.BlockSpec(memory_space=pltpu.VMEM),
            scratch_shapes=[
                vmem((own, width), bf16), vmem((width // LANES, LANES), bf16), vmem((own, 2 * HEAD), f32),
                vmem((2 * own, width), bf16), vmem((SLOTS, width, chunk), bf16), vmem((WO_SLOTS, wo_rows, width), bf16),
                vmem((2, 2 * own, chunk), bf16),
                vmem((heads * own, HEAD), bf16), vmem((heads // 2 * own, HEAD), bf16), vmem((kv_heads, tokens, 2 * HEAD), bf16),
                vmem((own, tokens), f32), vmem((2, own, wo_rows), bf16), vmem((own, width), f32),
                dma((kv_heads, n - 1)), dma((PIECES,)), dma((q_chunks,)),
            ],
            compiler_params=pltpu.CompilerParams(collective_id=0, has_side_effects=True, vmem_limit_bytes=52 * 2**20),
            cost_estimate=pl.CostEstimate(flops=2 * own * weights, bytes_accessed=2 * weights, transcendentals=heads * own * tokens),
        )(*(pltpu.with_memory_space_constraint(t, pltpu.HBM) for t in (x, gain.reshape(width // LANES, LANES), jnp.asarray(tables(tokens)), wq, wk, wv, wo)))

    rows, whole = P(("dp", "sp"), None), P(None, None)
    return jax.shard_map(
        step,
        mesh=mesh,
        in_specs=(rows, P(None), whole, whole, whole, whole),
        out_specs=rows,
        check_vma=False,
    )
```

```python
import functools

import jax
import jax.numpy as jnp
import numpy as np
from jax import lax
from jax.experimental import pallas as pl
from jax.experimental.pallas import tpu as pltpu
from jax.sharding import PartitionSpec as P

HEAD = 128
THETA = 10000
LOG2E = 1.4426950408889634
MESH = pl.DeviceIdType.MESH
LANES = 128
SLOTS = 5
WO_SLOTS = 5
PIECES = 1
N_COLS = 512
SENDS = [
    [(0, 0, 1), (0, 0, 3), (0, 1, 2), (0, 2, 3)],
    [(0, 0, 2), (1, 0, 3), (1, 2, 3)],
    [(1, 0, 1), (1, 1, 2)],
    [(2, 0, 3), (2, 1, 2), (1, 1, 3)],
    [(2, 0, 1), (1, 0, 2)],
    [(2, 2, 3), (3, 0, 3), (3, 0, 1), (2, 0, 2)],
    [(3, 1, 2), (3, 2, 3), (3, 0, 2), (3, 1, 3)],
    [],
]
RELAYS = {0: [(0, 2)], 1: [], 2: [], 3: [], 4: [(2, 2)]}
ORDER = [("s", 0), ("w", 0), ("w", 1), ("s", 1), ("w", 2), ("w", 3), ("p", 0), ("w", 4), ("w", 5), ("p", 1), ("w", 6), ("w", 7)]


def tables(tokens):
    half = HEAD // 2
    rate = np.float32(THETA) ** (-np.arange(half, dtype=np.float32) / np.float32(half))
    angle = (np.arange(tokens, dtype=np.float32)[:, None] * rate.astype(np.float32)).astype(np.float64)
    cos, sin = np.cos(angle).astype(np.float32), np.sin(angle).astype(np.float32)
    return np.concatenate([cos, cos, -sin, sin], -1)


def dot(a, b, ca=1, cb=0):
    return lax.dot_general(a, b, (((ca,), (cb,)), ((), ())), preferred_element_type=jnp.float32)


def kernel(n, x_hbm, gain_hbm, turn_hbm, wq_hbm, wk_hbm, wv_hbm, wo_hbm, y,
           x, gain, turn, a, w, wo, raw, q, q_out, kv, cap, seen, total,
           recv_sem, a_recv, q_recv, in_sem, kv_sem, w_sem, wo_sem, send_sem, relay_sem, a_send, q_send):
    me, group = lax.axis_index("sp"), lax.axis_index("dp")
    side = lax.rem(group, 2)
    partner = {"dp": group + 1 - 2 * side}
    own, width = x.shape
    kv_heads = kv.shape[0]
    heads = q.shape[0] // own
    per = heads // kv_heads
    chunk = w.shape[2]
    q_chunks = heads * HEAD // (2 * chunk)
    chunk_heads = chunk // HEAD
    chunks = 2 + q_chunks
    wo_rows = wo.shape[1]
    wo_chunks = heads * HEAD // wo_rows
    wo_per = wo_chunks // kv_heads
    tokens = n * own
    order = [lax.rem(kv_heads // 2 * side + k, kv_heads) for k in range(kv_heads)]

    def ds(at, size):
        return pl.ds(at if isinstance(at, int) else pl.multiple_of(at, size), size)

    mine = ds(me * own, own)

    place = pltpu.make_async_copy
    inputs = [
        place(x_hbm, x, in_sem.at[0]),
        place(gain_hbm, gain, in_sem.at[1]),
        place(turn_hbm.at[mine], turn, in_sem.at[2]),
    ]
    for c in inputs:
        c.start()

    def w_copy(i):
        return place(wq_hbm.at[:, ds((side * q_chunks + i - 2) * chunk, chunk)], w.at[i % SLOTS], w_sem.at[i])

    def kv_copy(i, k):
        return place((wk_hbm, wv_hbm)[i].at[:, ds(order[k] * HEAD, HEAD)], w.at[i, :, pl.ds(k * HEAD, HEAD)], kv_sem.at[i, k])

    def wo_copy(i):
        rows = ds(order[i // wo_per] * (wo_per * wo_rows) + i % wo_per * wo_rows, wo_rows)
        return place(wo_hbm.at[rows, :], wo.at[i % WO_SLOTS], wo_sem.at[i])

    def fetch(i):
        if i < chunks:
            w_copy(i).start(priority=1)

    for k in range(kv_heads):
        for i in range(2):
            kv_copy(i, k).start(priority=1)
    for i in range(2, SLOTS):
        fetch(i)

    barrier = pltpu.get_barrier_semaphore()
    for step in range(1, n):
        pl.semaphore_signal(barrier, inc=1, device_id={"sp": lax.rem(me + step, n)}, device_id_type=MESH)
    pl.semaphore_signal(barrier, inc=1, device_id=partner, device_id_type=MESH)

    def block(k, j):
        return kv.at[order[k], ds(j * own, own), :]

    for j in range(1, n):
        for k in range(kv_heads):
            @pl.when(me < j)
            def _():
                block(k, j)[...] = jnp.zeros((own, 2 * HEAD), kv.dtype)
    place_q = me * own + lax.broadcasted_iota(jnp.int32, (own, tokens), 0)
    place_k = lax.broadcasted_iota(jnp.int32, (own, tokens), 1)
    cap[...] = jnp.where(place_q >= place_k, jnp.inf, -jnp.inf)

    for c in inputs:
        c.wait()
    cols = [slice(i * LANES, (i + 1) * LANES) for i in range(width // LANES)]
    square = jnp.zeros((own, LANES), jnp.float32)
    for s in cols:
        wide = x[:, s].astype(jnp.float32)
        square += wide * wide
    scale = lax.rsqrt(jnp.sum(square, -1, keepdims=True) * (1 / width) + 1e-6)

    def a_copy(i):
        tall = own // PIECES
        return pltpu.make_async_remote_copy(src_ref=a.at[pl.ds(i * tall, tall)], dst_ref=a.at[pl.ds(own + i * tall, tall)], send_sem=a_send.at[i],
                                            recv_sem=a_recv.at[i], device_id=partner, device_id_type=MESH)

    for i, s in enumerate(cols):
        a[:own, s] = (x[:, s].astype(jnp.float32) * scale * gain[i : i + 1, :].astype(jnp.float32)).astype(a.dtype)

    def turned(t):
        t = t.astype(jnp.bfloat16).astype(jnp.float32)
        return (t * turn[:, :HEAD] + pltpu.roll(t, HEAD // 2, 1) * turn[:, HEAD:]).astype(jnp.bfloat16)

    def send(k, j, to, sem):
        return pltpu.make_async_remote_copy(src_ref=block(k, j), dst_ref=block(k, j), send_sem=sem, recv_sem=recv_sem.at[k, j],
                                            device_id={"sp": to}, device_id_type=MESH)

    hops = [(j, j + 1, range(kv_heads)) for j in range(n - 1)] + [(0, 3, range(kv_heads)), (0, 2, range(kv_heads)), (1, 3, [1, 3])]
    relays = [(2, 1, 3, [0, 2])]

    def first_hop(*what):
        for j in range(n - 1):
            to = [(k, t) for k, f, t in what if f == j]
            if to:
                @pl.when(me == j)
                def _():
                    for k, t in to:
                        send(k, j, t, send_sem.at[k, t]).start()

    for k in range(kv_heads):
        for i in range(2):
            kv_copy(i, k).wait()
        s = pl.ds(k * HEAD, HEAD)
        kv[order[k], mine, :HEAD] = turned(dot(a[:own], w[0, :, s]))
        kv[order[k], mine, HEAD:] = dot(a[:own], w[1, :, s]).astype(jnp.bfloat16)
        if k == 0:
            pl.semaphore_wait(barrier, n)
            for i in range(PIECES):
                a_copy(i).start()
        first_hop(*SENDS[k])
    for i in range(SLOTS, SLOTS + 2):
        fetch(i)

    def relay(what):
        for via, j, to, which in relays:
            for k in which:
                if (k, via) in what:
                    @pl.when(me == via)
                    def _():
                        send(k, j, to, relay_sem.at[k]).wait_recv()
                        send(k, j, to, relay_sem.at[k]).start()

    def q_copy(i, whose):
        rows = pl.ds(i * chunk_heads * own, chunk_heads * own)
        there = ds((whose * q_chunks + i) * (chunk_heads * own), chunk_heads * own)
        return pltpu.make_async_remote_copy(src_ref=q_out.at[rows], dst_ref=q.at[there], send_sem=q_send.at[i], recv_sem=q_recv.at[i],
                                            device_id=partner, device_id_type=MESH)

    def turn_queries(i):
        for u in range(chunk_heads):
            s = slice(u * HEAD, (u + 1) * HEAD)
            h = i * chunk_heads + u
            q_out[h * own : (h + 1) * own, :] = turned(raw[i % 2, own:, s])
            q[ds((side * (heads // 2) + h) * own, own), :] = turned(raw[i % 2, :own, s])

    for i in range(q_chunks):
        w_copy(2 + i).wait()
        if i == 0:
            raw[i % 2, :own] = dot(a[:own], w[(2 + i) % SLOTS]).astype(raw.dtype)
            for c in range(PIECES):
                a_copy(c).wait_recv()
            raw[i % 2, own:] = dot(a[own:], w[(2 + i) % SLOTS]).astype(raw.dtype)
        else:
            raw[i % 2] = dot(a[...], w[(2 + i) % SLOTS]).astype(raw.dtype)
        if i > 0:
            turn_queries(i - 1)
            q_copy(i - 1, side).start()
        for c in ([0, 1], [2], [3], [4])[i]:
            wo_copy(c).start(priority=1)
        relay(RELAYS[i])
        first_hop(*SENDS[kv_heads + i])

    e = HEAD**-0.5 * LOG2E
    heads_at_once = 2
    strip = heads_at_once * own
    strips = wo_rows // (heads_at_once * HEAD)

    def output(j, c):
        s = pl.ds(c * N_COLS, N_COLS)
        t = dot(seen[j % 2], wo[j % WO_SLOTS, :, s])
        if j == 0:
            total[:, s] = t
        elif j < wo_chunks - 1:
            total[:, s] += t
        else:
            y[:, s] = (x[:, s].astype(jnp.float32) + (total[:, s] + t)).astype(y.dtype)

    pieces = width // N_COLS
    def attend(seen_blocks):
        in_view = seen_blocks * own
        for j in range(wo_chunks):
            k = j // wo_per
            if j % wo_per == 0:
                for b in range(seen_blocks - 1):
                    ok = me > b
                    for via, of, _, which in relays:
                        if of == b and k in which:
                            ok = ok & (me != via)
                    @pl.when(ok)
                    def _():
                        send(k, b, lax.rem(me + 1, n), relay_sem.at[k]).wait_recv()
                if k >= kv_heads // 2:
                    of = per // chunk_heads
                    for i in range((k - kv_heads // 2) * of, (k - kv_heads // 2 + 1) * of):
                        q_copy(i, 1 - side).wait_recv()
            if j > 0:
                wo_copy(j - 1).wait()
            else:
                turn_queries(q_chunks - 1)
            keys = kv[order[k], :in_view, :HEAD]
            values = jnp.concatenate([kv[order[k], :in_view, HEAD:], jnp.ones((in_view, HEAD), kv.dtype)], axis=1)
            scores = {}
            for kind, u in ORDER:
                if kind == "s":
                    at = (order[k] * wo_per + j % wo_per) * strips + u
                    scores[u] = dot(q[ds(at * strip, strip), :], keys, 1, 1)
                elif kind == "w":
                    if j > 0:
                        output(j - 1, u)
                else:
                    s = jnp.minimum(scores[u], jnp.concatenate([cap[:, :in_view]] * heads_at_once, axis=0))
                    top = jnp.max(s, -1, keepdims=True)
                    p = jnp.exp2((s - top) * e).astype(jnp.bfloat16)
                    o = dot(p, values)
                    o = (o[:, :HEAD] / o[:, HEAD:]).astype(jnp.bfloat16)
                    for v in range(heads_at_once):
                        h = u * heads_at_once + v
                        seen[j % 2, :, h * HEAD : (h + 1) * HEAD] = o[v * own : (v + 1) * own, :]
            if j == 0:
                q_copy(q_chunks - 1, side).start()
            elif j - 1 + WO_SLOTS < wo_chunks:
                wo_copy(j - 1 + WO_SLOTS).start(priority=1)
            relay(RELAYS.get(q_chunks + j, []))

    pl.when(me == 0)(lambda: attend(1))
    pl.when(me != 0)(lambda: attend(n))
    wo_copy(wo_chunks - 1).wait()
    for c in range(pieces):
        output(wo_chunks - 1, c)

    for i in range(PIECES):
        a_copy(i).wait_send()
    for i in range(q_chunks):
        q_copy(i, side).wait_send()
    for j, to, which in hops:
        @pl.when(me == j)
        def _():
            for k in which:
                send(k, j, to, send_sem.at[k, to]).wait_send()
    for via, j, to, which in relays:
        @pl.when(me == via)
        def _():
            for k in which:
                send(k, j, to, relay_sem.at[k]).wait_send()


def scoped(n, semaphores, *refs):
    pl.run_scoped(lambda *local: kernel(n, *refs, *local), *semaphores)


def solution(mesh):
    n = mesh.shape["sp"]

    def step(x, gain, wq, wk, wv, wo):
        own, width = x.shape
        kv_heads, heads = wk.shape[1] // HEAD, wq.shape[1] // HEAD
        chunk = wk.shape[1]
        q_chunks = wq.shape[1] // (2 * chunk)
        tokens = n * own
        wo_rows = 512
        wo_chunks = wo.shape[0] // wo_rows
        anywhere = pl.BlockSpec(memory_space=pltpu.HBM)
        weights = sum(t.size for t in (wq, wk, wv, wo))
        vmem, f32, bf16, dma = pltpu.VMEM, jnp.float32, jnp.bfloat16, pltpu.SemaphoreType.DMA
        local = [dma((3,)), dma((2, kv_heads)), dma((2 + q_chunks,)), dma((wo_chunks,)), dma((kv_heads, n)), dma((kv_heads,)), dma((PIECES,)),
                 dma((q_chunks,))]
        return pl.pallas_call(
            functools.partial(scoped, n, local),
            out_shape=jax.ShapeDtypeStruct(x.shape, x.dtype),
            in_specs=[anywhere] * 7,
            out_specs=pl.BlockSpec(memory_space=pltpu.VMEM),
            scratch_shapes=[
                vmem((own, width), bf16), vmem((width // LANES, LANES), bf16), vmem((own, 2 * HEAD), f32),
                vmem((2 * own, width), bf16), vmem((SLOTS, width, chunk), bf16), vmem((WO_SLOTS, wo_rows, width), bf16),
                vmem((2, 2 * own, chunk), bf16),
                vmem((heads * own, HEAD), bf16), vmem((heads // 2 * own, HEAD), bf16), vmem((kv_heads, tokens, 2 * HEAD), bf16),
                vmem((own, tokens), f32), vmem((2, own, wo_rows), bf16), vmem((own, width), f32),
                dma((kv_heads, n - 1)), dma((PIECES,)), dma((q_chunks,)),
            ],
            compiler_params=pltpu.CompilerParams(collective_id=0, has_side_effects=True, vmem_limit_bytes=52 * 2**20),
            cost_estimate=pl.CostEstimate(flops=2 * own * weights, bytes_accessed=2 * weights, transcendentals=heads * own * tokens),
        )(*(pltpu.with_memory_space_constraint(t, pltpu.HBM) for t in (x, gain.reshape(width // LANES, LANES), jnp.asarray(tables(tokens)), wq, wk, wv, wo)))

    rows, whole = P(("dp", "sp"), None), P(None, None)
    return jax.shard_map(
        step,
        mesh=mesh,
        in_specs=(rows, P(None), whole, whole, whole, whole),
        out_specs=rows,
        check_vma=False,
    )
```
